32 devices in a mesh: lat: 4 (over z), lon: 4 (over y, x), lev: 2 (over core).
Axes of the slice: x: 2, y: 2, z: 4, core: 2. Of those that a mesh axis runs over, the one named last changes fastest.
Arguments:
- initial_heat: float32 [64, 32, 192, 128], P('lat', 'lon', 'lev'), may hold values from 0.2 to 1.8
- scaled_wind_north: float32 [64, 32, 192, 128], P('lat', 'lon', 'lev'), may hold values from -0.3 to 0.3
- scaled_wind_east: float32 [64, 32, 192, 128], P('lat', 'lon', 'lev'), may hold values from -0.3 to 0.3
- scaled_wind_vertical: float32 [64, 32, 192, 128], P('lat', 'lon', 'lev'), may hold values from -0.3 to 0.3
Outputs:
- accumulated_eastward: float32 [64, 32, 192, 128], P('lat', 'lon', 'lev')
- temperature_end: float32 [64, 32, 192, 128], P('lat', 'lon', 'lev')
The draws below stay inside these ranges and needn't reach their ends.
All inputs are finite; a program needn't handle non-finite values.
Results may differ from the reference program's by a relative error of at most 0.00002.
Values sent between devices are 32-bit elements; how exact they have to be, the bound alone decides.
A program may use at most 448 MiB of HBM per device.

```python
import jax
import jax.numpy as jnp
from jax import lax

NORTHWARD_BOXES = 64
EASTWARD_BOXES = 32
UPWARD_BOXES = 192
LAYER_TOTAL = 128
STEPS = 6


def levels(own_key, shape, pieces, least, high):
    def one(dim, blocks):
        draws = jax.random.uniform(jax.random.fold_in(jax.random.fold_in(own_key, 6), dim), (blocks,), jnp.float32, least / len(pieces), high / len(pieces))
        return jnp.repeat(jnp.exp(draws), shape[dim] // blocks).reshape((-1,) + (1,) * (len(shape) - dim - 1))

    factor_of = one(*pieces[0])
    for cut in pieces[1:]:
        factor_of = factor_of * one(*cut)
    return factor_of


def setup_inputs(seed: int = 0) -> dict:
    key_list = jax.random.split(jax.random.key(seed), 5)
    return {
        "initial_heat": jnp.clip(0.2 + 1.5999999 * jax.random.uniform(key_list[0], (NORTHWARD_BOXES, EASTWARD_BOXES, UPWARD_BOXES, LAYER_TOTAL), jnp.float32) ** levels(key_list[0], (NORTHWARD_BOXES, EASTWARD_BOXES, UPWARD_BOXES, LAYER_TOTAL), ((0, 4), (1, 4), (2, 2)), -0.2, 0.2), 0.2, 1.8),
        "scaled_wind_north": jnp.clip(jax.random.uniform(key_list[1], (NORTHWARD_BOXES, EASTWARD_BOXES, UPWARD_BOXES, LAYER_TOTAL), jnp.float32, -0.3, 0.3) * levels(key_list[1], (NORTHWARD_BOXES, EASTWARD_BOXES, UPWARD_BOXES, LAYER_TOTAL), ((0, 4), (1, 4), (2, 2)), -0.4, 0.0), -0.3, 0.3),
        "scaled_wind_east": jnp.clip(jax.random.uniform(key_list[2], (NORTHWARD_BOXES, EASTWARD_BOXES, UPWARD_BOXES, LAYER_TOTAL), jnp.float32, -0.3, 0.3) * levels(key_list[2], (NORTHWARD_BOXES, EASTWARD_BOXES, UPWARD_BOXES, LAYER_TOTAL), ((0, 4), (1, 4), (2, 2)), -0.4, 0.0), -0.3, 0.3),
        "scaled_wind_vertical": jnp.clip(jax.random.uniform(key_list[3], (NORTHWARD_BOXES, EASTWARD_BOXES, UPWARD_BOXES, LAYER_TOTAL), jnp.float32, -0.3, 0.3) * levels(key_list[3], (NORTHWARD_BOXES, EASTWARD_BOXES, UPWARD_BOXES, LAYER_TOTAL), ((0, 4), (1, 4), (2, 2)), -0.4, 0.0), -0.3, 0.3),
    }


def strip_edges(values, dims):
    for dim in dims:
        values = lax.slice_in_dim(values, 1, values.shape[dim] - 1, axis=dim)
    return values


def neighbour(values, dim, start, dims):
    others = [other for other in dims if other != dim]
    values = strip_edges(values, others)
    return lax.slice_in_dim(values, start, start + values.shape[dim] - 2, axis=dim)


def single_update(extended_field, scaled_wind_north, scaled_wind_east, scaled_wind_vertical):
    middle = strip_edges(extended_field, (0, 1, 2))
    lower = [neighbour(extended_field, dim, 0, (0, 1, 2)) for dim in (0, 1, 2)]
    upper = [neighbour(extended_field, dim, 2, (0, 1, 2)) for dim in (0, 1, 2)]
    slopes = [above - beneath_layer for above, beneath_layer in zip(upper, lower)]
    smooth_rate = 0.05
    spread = lower[0] + upper[0] + lower[1] + upper[1] + lower[2] + upper[2] - 6.0 * middle
    return middle - scaled_wind_north * slopes[0] - scaled_wind_east * slopes[1] - scaled_wind_vertical * slopes[2] + smooth_rate * spread


def reference(initial_heat, scaled_wind_north, scaled_wind_east, scaled_wind_vertical):
    for step in range(STEPS):
        initial_heat = single_update(jnp.pad(initial_heat, ((1, 1), (1, 1), (1, 1), (0, 0)), mode="constant"), scaled_wind_north, scaled_wind_east, scaled_wind_vertical)
    accumulated_eastward = jnp.cumsum(initial_heat, axis=1) / EASTWARD_BOXES
    return accumulated_eastward, initial_heat
```

```python
import functools

import jax
import jax.numpy as jnp
from jax import lax
from jax.experimental import pallas as pl
from jax.experimental.pallas import tpu as pltpu
from jax.sharding import PartitionSpec as P

STEPS = 6
RATE = 0.05
LAG = 1
TOTAL_LAG = 4
RELAY = False
RELAY_FIRST_DIM = True
MESH = pl.DeviceIdType.MESH


def relay_routes(mesh):
    if not RELAY:
        return ()
    row = mesh.devices[0, :, 0]
    spots = [getattr(device, "coords", None) for device in row]
    if any(spot is None for spot in spots):
        return ()
    spots = [tuple(spot) for spot in spots]
    routes = []
    for low in range(len(spots) - 1):
        for source, target, side in ((low, low + 1, 0), (low + 1, low, 1)):
            a, b = spots[source], spots[target]
            differ = [d for d in range(3) if a[d] != b[d]]
            if len(differ) != 2:
                continue
            keep, change = differ if RELAY_FIRST_DIM else differ[::-1]
            corner = list(a)
            corner[change] = b[change]
            if tuple(corner) in spots:
                routes.append((source, spots.index(tuple(corner)), target, side))
    return tuple(routes)


def march(routes, sizes, heat, north, east, vert, end_out, enter_out,
          T, W, zh, zs, tot, ent, rbuf,
          load_sem, xs_sem, xr_sem, ys_sem, yr_sem, zs_sem, zr_sem,
          rs_in_sem, rr_sem, rs_sem, ts_sem, tr_sem, out_sem, enter_sem):
    lats, lons, levs = sizes
    Y, X, Z, L = heat.shape
    pairs = Y // 2
    lat, lon, lev = (lax.axis_index(a) for a in ("lat", "lon", "lev"))
    winds = (north, east, vert)

    def remote(src, dst, send, recv, where):
        return pltpu.make_async_remote_copy(
            src_ref=src, dst_ref=dst, send_sem=send, recv_sem=recv,
            device_id=where, device_id_type=MESH)

    def load(j, k):
        if k == 3:
            return pltpu.make_async_copy(heat.at[j], T.at[0, 1 + j, pl.ds(1, X)], load_sem.at[3, j])
        return pltpu.make_async_copy(winds[k].at[j], W.at[k, j], load_sem.at[k, j])

    def start_loads(p, _):
        for k in range(3):
            load(p, k).start()
            load(Y - 1 - p, k).start()
        return 0

    def start_heat(j, _):
        load(j, 3).start()
        return 0

    lax.fori_loop(0, Y, start_heat, 0)
    lax.fori_loop(0, pairs, start_loads, 0)

    @pl.when(lon == 0)
    def _():
        T[:, pl.ds(1, Y), 0] = jnp.zeros((2, Y, Z, L), jnp.float32)

    @pl.when(lon == lons - 1)
    def _():
        T[:, pl.ds(1, Y), X + 1] = jnp.zeros((2, Y, Z, L), jnp.float32)

    @pl.when(lat == 0)
    def _():
        T[:, 0, pl.ds(1, X)] = jnp.zeros((2, X, Z, L), jnp.float32)

    @pl.when(lat == lats - 1)
    def _():
        T[:, Y + 1, pl.ds(1, X)] = jnp.zeros((2, X, Z, L), jnp.float32)

    @pl.when(lev == 0)
    def _():
        zh[:, 0] = jnp.zeros((2, Y, X, L), jnp.float32)

    @pl.when(lev == levs - 1)
    def _():
        zh[:, 1] = jnp.zeros((2, Y, X, L), jnp.float32)

    barrier = pltpu.get_barrier_semaphore()
    expected = jnp.int32(0)
    for axis, place, count in (("lat", lat, lats), ("lon", lon, lons), ("lev", lev, levs)):
        for cond, other in ((place > 0, place - 1), (place < count - 1, place + 1)):
            @pl.when(cond)
            def _(axis=axis, other=other):
                pl.semaphore_signal(barrier, inc=1, device_id={axis: other}, device_id_type=MESH)
            expected = expected + jnp.where(cond, 1, 0)
    met = set()
    for source, relay, target, _ in routes:
        for a, b in ((source, relay), (relay, target)):
            link = (min(a, b), max(a, b))
            if link[1] - link[0] == 1 or link in met:
                continue
            met.add(link)
            for me, other in (link, link[::-1]):
                @pl.when(lon == me)
                def _(other=other):
                    pl.semaphore_signal(barrier, inc=1, device_id={"lon": jnp.int32(other)}, device_id_type=MESH)
                expected = expected + jnp.where(lon == me, 1, 0)
    pl.semaphore_wait(barrier, expected)

    def x_copy(slot, side, j, src):
        land = 0 if side == 0 else X + 1
        other = lon + 1 if side == 0 else lon - 1
        return remote(src, T.at[slot, 1 + j, land], xs_sem.at[slot, side, j],
                      xr_sem.at[slot, side, j], {"lon": other})

    def has_target(side):
        return lon < lons - 1 if side == 0 else lon > 0

    def has_source(side):
        return lon > 0 if side == 0 else lon < lons - 1

    def on_route(side, relayed):
        hit = False
        if relayed:
            for source, _, _, s in routes:
                if s == side:
                    hit = jnp.logical_or(hit, lon == source)
        return hit

    def send_x(step, slot, j, p, relayed, srcs):
        for side in (0, 1):
            routed = on_route(side, relayed)

            @pl.when(jnp.logical_and(has_target(side), jnp.logical_not(routed)))
            def _(side=side):
                x_copy(slot, side, j, srcs[side]).start()

        if relayed:
            for number, (source, relay, target, side) in enumerate(routes):
                @pl.when(lon == source)
                def _(relay=relay, side=side):
                    remote(srcs[side], rbuf.at[step, p], xs_sem.at[slot, side, j],
                           rr_sem.at[step, p], {"lon": jnp.int32(relay)}).start()

    def wait_send_x(slot, j):
        for side in (0, 1):
            @pl.when(has_target(side))
            def _(side=side):
                x_copy(slot, side, j, T.at[slot, 1 + j, X if side == 0 else 1]).wait_send()

    def wait_recv_x(slot, j):
        for side in (0, 1):
            @pl.when(has_source(side))
            def _(side=side):
                x_copy(slot, side, j, T.at[slot, 1 + j, X if side == 0 else 1]).wait_recv()

    def relay_copy(step, p, target, side):
        slot = lax.rem(step, 2)
        j = Y - 1 - p
        land = 0 if side == 0 else X + 1
        return remote(rbuf.at[step, p], T.at[slot, 1 + j, land], rs_sem.at[step, p],
                      xr_sem.at[slot, side, j], {"lon": jnp.int32(target)})

    def do_relay(step, p):
        for source, relay, target, side in routes:
            @pl.when(lon == relay)
            def _(target=target, side=side):
                remote(rbuf.at[step, p], rbuf.at[step, p], rs_in_sem.at[0],
                       rr_sem.at[step, p], {"lon": jnp.int32(target)}).wait_recv()
                relay_copy(step, p, target, side).start()

    def y_copy(slot, side):
        if side == 0:
            return remote(T.at[slot, Y, pl.ds(1, X)], T.at[slot, 0, pl.ds(1, X)],
                          ys_sem.at[slot, 0], yr_sem.at[slot, 0], {"lat": lat + 1})
        return remote(T.at[slot, 1, pl.ds(1, X)], T.at[slot, Y + 1, pl.ds(1, X)],
                      ys_sem.at[slot, 1], yr_sem.at[slot, 1], {"lat": lat - 1})

    def y_target(side):
        return lat < lats - 1 if side == 0 else lat > 0

    def y_source(side):
        return lat > 0 if side == 0 else lat < lats - 1

    def z_copy(slot, side, j):
        other = lev + 1 if side == 0 else lev - 1
        return remote(zs.at[slot, side, j], zh.at[slot, side, j], zs_sem.at[slot, side, j],
                      zr_sem.at[slot, side, j], {"lev": other})

    def z_target(side):
        return lev < levs - 1 if side == 0 else lev > 0

    def z_source(side):
        return lev > 0 if side == 0 else lev < levs - 1

    def send_z(slot, j):
        for side in (0, 1):
            @pl.when(z_target(side))
            def _(side=side):
                z_copy(slot, side, j).start()

    def wait_send_z(slot, j):
        for side in (0, 1):
            @pl.when(z_target(side))
            def _(side=side):
                z_copy(slot, side, j).wait_send()

    def wait_recv_z(slot, j):
        for side in (0, 1):
            @pl.when(z_source(side))
            def _(side=side):
                z_copy(slot, side, j).wait_recv()

    def first_x(p, _):
        for j, relayed in ((p, False), (Y - 1 - p, True)):
            send_x(0, 0, j, p, relayed, (heat.at[j, X - 1], heat.at[j, 0]))
        return 0

    lax.fori_loop(0, pairs, first_x, 0)

    def wait_heat(j, _):
        load(j, 3).wait()
        return 0

    lax.fori_loop(0, Y, wait_heat, 0)
    for side in (0, 1):
        @pl.when(y_target(side))
        def _(side=side):
            y_copy(0, side).start()

    def first_z(j, _):
        for x in range(X):
            zs[0, 0, j, pl.ds(x, 1)] = T[0, 1 + j, 1 + x, pl.ds(Z - 1, 1)]
            zs[0, 1, j, pl.ds(x, 1)] = T[0, 1 + j, 1 + x, pl.ds(0, 1)]
        return 0

    lax.fori_loop(0, Y, first_z, 0)

    def first_z_send(j, _):
        send_z(0, j)
        return 0

    lax.fori_loop(0, Y, first_z_send, 0)

    level = lax.broadcasted_iota(jnp.int32, (Z, L), 0)

    def update(old, j, with_total):
        new = 1 - old
        total = None
        for x in range(X):
            c = T[old, 1 + j, 1 + x]
            ym, yp = T[old, j, 1 + x], T[old, j + 2, 1 + x]
            xm, xp = T[old, 1 + j, x], T[old, 1 + j, x + 2]
            zm = jnp.where(level == 0, zh[old, 0, j, pl.ds(x, 1)], pltpu.roll(c, 1, 0))
            zp = jnp.where(level == Z - 1, zh[old, 1, j, pl.ds(x, 1)], pltpu.roll(c, Z - 1, 0))
            spread = ym + yp + xm + xp + zm + zp - 6.0 * c
            value = (c - W[0, j, x] * (yp - ym) - W[1, j, x] * (xp - xm)
                     - W[2, j, x] * (zp - zm) + RATE * spread)
            T[new, 1 + j, 1 + x] = value
            if not with_total:
                zs[new, 0, j, pl.ds(x, 1)] = value[Z - 1:Z]
                zs[new, 1, j, pl.ds(x, 1)] = value[0:1]
            elif total is None:
                total = value
            else:
                total = total + value
        if with_total:
            tot[j] = total

    def arrivals(old, j, p, edge_side):
        wait_recv_x(old, j)
        wait_recv_z(old, j)

        @pl.when(jnp.logical_and(p == 0, y_source(edge_side)))
        def _():
            y_copy(old, edge_side).wait_recv()

    def departures(slot, j, p, edge_side):
        wait_send_x(slot, j)
        wait_send_z(slot, j)

        @pl.when(jnp.logical_and(p == 0, y_target(edge_side)))
        def _():
            y_copy(slot, edge_side).wait_send()

    def one_pair(q, _):
        step = q // pairs
        p = lax.rem(q, pairs)
        old = lax.rem(step, 2)
        new = 1 - old

        @pl.when(step == 0)
        def _():
            do_relay(0, p)
            for k in range(3):
                load(p, k).wait()
                load(Y - 1 - p, k).wait()

        for j, edge_side, relayed in ((p, 0, False), (Y - 1 - p, 1, True)):
            arrivals(old, j, p, edge_side)

            @pl.when(step > 0)
            def _(j=j, edge_side=edge_side):
                departures(new, j, p, 1 - edge_side)

            update(old, j, False)
            send_x(step + 1, new, j, p, relayed, (T.at[new, 1 + j, X], T.at[new, 1 + j, 1]))
            send_z(new, j)

            @pl.when(jnp.logical_and(p == 0, y_target(1 - edge_side)))
            def _(edge_side=edge_side):
                y_copy(new, 1 - edge_side).start()

        late = q - LAG

        @pl.when(late >= 0)
        def _():
            do_relay(late // pairs + 1, lax.rem(late, pairs))

        return 0

    lax.fori_loop(0, (STEPS - 1) * pairs, one_pair, 0)

    old = (STEPS - 1) % 2
    new = 1 - old

    def out_copy(j):
        return pltpu.make_async_copy(T.at[new, 1 + j, pl.ds(1, X)], end_out.at[j], out_sem.at[j])

    def t_copy(j):
        return remote(tot.at[j], ent.at[j], ts_sem.at[j], tr_sem.at[j], {"lon": lon + 1})

    def enter_copy(j):
        return pltpu.make_async_copy(ent.at[j], enter_out.at[j], enter_sem.at[j])

    def pass_total(p):
        for j in (p, Y - 1 - p):
            @pl.when(lon > 0)
            def _(j=j):
                t_copy(j).wait_recv()

                @pl.when(lon < lons - 1)
                def _():
                    tot[j] = tot[j] + ent[j]
                    t_copy(j).start()

            enter_copy(j).start()

    def clear_enter(j, _):
        ent[j] = jnp.zeros((Z, L), jnp.float32)
        return 0

    @pl.when(lon == 0)
    def _():
        lax.fori_loop(0, Y, clear_enter, 0)

    def leftover(p, _):
        do_relay(STEPS - 1, p)
        return 0

    lax.fori_loop(pairs - LAG, pairs, leftover, 0)

    def last_pair(p, _):
        for j, edge_side in ((p, 0), (Y - 1 - p, 1)):
            arrivals(old, j, p, edge_side)
            departures(new, j, p, 1 - edge_side)
            update(old, j, True)
        for j in (p, Y - 1 - p):
            @pl.when(jnp.logical_and(lon == 0, lons > 1))
            def _(j=j):
                t_copy(j).start()

            out_copy(j).start()

        @pl.when(p >= TOTAL_LAG)
        def _():
            pass_total(p - TOTAL_LAG)

        return 0

    lax.fori_loop(0, pairs, last_pair, 0)

    def last_totals(p, _):
        pass_total(p)
        return 0

    lax.fori_loop(max(pairs - TOTAL_LAG, 0), pairs, last_totals, 0)

    def drain(j, _):
        wait_send_x(old, j)
        wait_send_z(old, j)

        @pl.when(lon < lons - 1)
        def _():
            t_copy(j).wait_send()

        out_copy(j).wait()
        enter_copy(j).wait()
        return 0

    lax.fori_loop(0, Y, drain, 0)
    for side in (0, 1):
        @pl.when(y_target(side))
        def _(side=side):
            y_copy(old, side).wait_send()

    for source, relay, target, side in routes:
        def close(p, _, target=target, side=side):
            for step in range(STEPS):
                relay_copy(step, p, target, side).wait_send()
            return 0

        @pl.when(lon == relay)
        def _(close=close):
            lax.fori_loop(0, pairs, close, 0)


def integrate(scale, end_ref, enter_ref, acc_ref, copy_ref):
    X = end_ref.shape[1]
    running = enter_ref[0]
    for x in range(X):
        value = end_ref[0, x]
        copy_ref[0, x] = value
        running = running + value
        acc_ref[0, x] = running * scale


def per_device(routes, sizes, heat, north, east, vert):
    Y, X, Z, L = heat.shape
    pairs = Y // 2
    f32 = jnp.float32
    any_spec = pl.BlockSpec(memory_space=pl.ANY)
    dma = pltpu.SemaphoreType.DMA
    relay_rows = (STEPS, pairs) if routes else (1, 1)
    end, enter = pl.pallas_call(
        functools.partial(march, routes, sizes),
        out_shape=(jax.ShapeDtypeStruct((Y, X, Z, L), f32), jax.ShapeDtypeStruct((Y, Z, L), f32)),
        in_specs=[any_spec] * 4,
        out_specs=(any_spec, any_spec),
        scratch_shapes=[
            pltpu.VMEM((2, Y + 2, X + 2, Z, L), f32),
            pltpu.VMEM((3, Y, X, Z, L), f32),
            pltpu.VMEM((2, 2, Y, X, L), f32),
            pltpu.VMEM((2, 2, Y, X, L), f32),
            pltpu.VMEM((Y, Z, L), f32),
            pltpu.VMEM((Y, Z, L), f32),
            pltpu.VMEM(relay_rows + (Z, L), f32),
            dma((4, Y)),
            dma((2, 2, Y)), dma((2, 2, Y)),
            dma((2, 2)), dma((2, 2)),
            dma((2, 2, Y)), dma((2, 2, Y)),
            dma((1,)), dma(relay_rows), dma(relay_rows),
            dma((Y,)), dma((Y,)), dma((Y,)), dma((Y,)),
        ],
        compiler_params=pltpu.CompilerParams(
            collective_id=0, has_side_effects=True, vmem_limit_bytes=62 * 1024 * 1024),
        name="march",
    )(heat, north, east, vert)
    row = pl.BlockSpec((1, X, Z, L), lambda j: (j, 0, 0, 0))
    return pl.pallas_call(
        functools.partial(integrate, 1.0 / (X * sizes[1])),
        grid=(Y,),
        in_specs=[row, pl.BlockSpec((1, Z, L), lambda j: (j, 0, 0))],
        out_specs=(row, row),
        out_shape=(jax.ShapeDtypeStruct((Y, X, Z, L), f32),) * 2,
        name="integrate",
    )(end, enter)


def solution(mesh):
    spec = P("lat", "lon", "lev", None)
    sizes = tuple(mesh.shape[a] for a in ("lat", "lon", "lev"))
    return jax.shard_map(
        functools.partial(per_device, relay_routes(mesh), sizes),
        mesh=mesh, in_specs=(spec,) * 4, out_specs=(spec, spec), check_vma=False)
```

```python
import functools

import jax
import jax.numpy as jnp
from jax import lax
from jax.experimental import pallas as pl
from jax.experimental.pallas import tpu as pltpu
from jax.sharding import PartitionSpec as P

STEPS = 6
RATE = 0.05
LAG = 1
TOTAL_LAG = 4
RELAY = True
RELAY_FIRST_DIM = True
MESH = pl.DeviceIdType.MESH


def relay_routes(mesh):
    if not RELAY:
        return ()
    row = mesh.devices[0, :, 0]
    spots = [getattr(device, "coords", None) for device in row]
    if any(spot is None for spot in spots):
        return ()
    spots = [tuple(spot) for spot in spots]
    routes = []
    for low in range(len(spots) - 1):
        for source, target, side in ((low, low + 1, 0), (low + 1, low, 1)):
            a, b = spots[source], spots[target]
            differ = [d for d in range(3) if a[d] != b[d]]
            if len(differ) != 2:
                continue
            keep, change = differ if RELAY_FIRST_DIM else differ[::-1]
            corner = list(a)
            corner[change] = b[change]
            if tuple(corner) in spots:
                routes.append((source, spots.index(tuple(corner)), target, side))
    return tuple(routes)


def march(routes, sizes, heat, north, east, vert, end_out, enter_out,
          T, W, zh, zs, tot, ent, rbuf,
          load_sem, xs_sem, xr_sem, ys_sem, yr_sem, zs_sem, zr_sem,
          rs_in_sem, rr_sem, rs_sem, ts_sem, tr_sem, out_sem, enter_sem):
    lats, lons, levs = sizes
    Y, X, Z, L = heat.shape
    pairs = Y // 2
    lat, lon, lev = (lax.axis_index(a) for a in ("lat", "lon", "lev"))
    winds = (north, east, vert)

    def remote(src, dst, send, recv, where):
        return pltpu.make_async_remote_copy(
            src_ref=src, dst_ref=dst, send_sem=send, recv_sem=recv,
            device_id=where, device_id_type=MESH)

    def load(j, k):
        if k == 3:
            return pltpu.make_async_copy(heat.at[j], T.at[0, 1 + j, pl.ds(1, X)], load_sem.at[3, j])
        return pltpu.make_async_copy(winds[k].at[j], W.at[k, j], load_sem.at[k, j])

    def start_loads(p, _):
        for k in range(3):
            load(p, k).start()
            load(Y - 1 - p, k).start()
        return 0

    def start_heat(j, _):
        load(j, 3).start()
        return 0

    lax.fori_loop(0, Y, start_heat, 0)
    lax.fori_loop(0, pairs, start_loads, 0)

    @pl.when(lon == 0)
    def _():
        T[:, pl.ds(1, Y), 0] = jnp.zeros((2, Y, Z, L), jnp.float32)

    @pl.when(lon == lons - 1)
    def _():
        T[:, pl.ds(1, Y), X + 1] = jnp.zeros((2, Y, Z, L), jnp.float32)

    @pl.when(lat == 0)
    def _():
        T[:, 0, pl.ds(1, X)] = jnp.zeros((2, X, Z, L), jnp.float32)

    @pl.when(lat == lats - 1)
    def _():
        T[:, Y + 1, pl.ds(1, X)] = jnp.zeros((2, X, Z, L), jnp.float32)

    @pl.when(lev == 0)
    def _():
        zh[:, 0] = jnp.zeros((2, Y, X, L), jnp.float32)

    @pl.when(lev == levs - 1)
    def _():
        zh[:, 1] = jnp.zeros((2, Y, X, L), jnp.float32)

    barrier = pltpu.get_barrier_semaphore()
    expected = jnp.int32(0)
    for axis, place, count in (("lat", lat, lats), ("lon", lon, lons), ("lev", lev, levs)):
        for cond, other in ((place > 0, place - 1), (place < count - 1, place + 1)):
            @pl.when(cond)
            def _(axis=axis, other=other):
                pl.semaphore_signal(barrier, inc=1, device_id={axis: other}, device_id_type=MESH)
            expected = expected + jnp.where(cond, 1, 0)
    met = set()
    for source, relay, target, _ in routes:
        for a, b in ((source, relay), (relay, target)):
            link = (min(a, b), max(a, b))
            if link[1] - link[0] == 1 or link in met:
                continue
            met.add(link)
            for me, other in (link, link[::-1]):
                @pl.when(lon == me)
                def _(other=other):
                    pl.semaphore_signal(barrier, inc=1, device_id={"lon": jnp.int32(other)}, device_id_type=MESH)
                expected = expected + jnp.where(lon == me, 1, 0)
    pl.semaphore_wait(barrier, expected)

    def x_copy(slot, side, j, src):
        land = 0 if side == 0 else X + 1
        other = lon + 1 if side == 0 else lon - 1
        return remote(src, T.at[slot, 1 + j, land], xs_sem.at[slot, side, j],
                      xr_sem.at[slot, side, j], {"lon": other})

    def has_target(side):
        return lon < lons - 1 if side == 0 else lon > 0

    def has_source(side):
        return lon > 0 if side == 0 else lon < lons - 1

    def on_route(side, relayed):
        hit = False
        if relayed:
            for source, _, _, s in routes:
                if s == side:
                    hit = jnp.logical_or(hit, lon == source)
        return hit

    def send_x(step, slot, j, p, relayed, srcs):
        for side in (0, 1):
            routed = on_route(side, relayed)

            @pl.when(jnp.logical_and(has_target(side), jnp.logical_not(routed)))
            def _(side=side):
                x_copy(slot, side, j, srcs[side]).start()

        if relayed:
            for number, (source, relay, target, side) in enumerate(routes):
                @pl.when(lon == source)
                def _(relay=relay, side=side):
                    remote(srcs[side], rbuf.at[step, p], xs_sem.at[slot, side, j],
                           rr_sem.at[step, p], {"lon": jnp.int32(relay)}).start()

    def wait_send_x(slot, j):
        for side in (0, 1):
            @pl.when(has_target(side))
            def _(side=side):
                x_copy(slot, side, j, T.at[slot, 1 + j, X if side == 0 else 1]).wait_send()

    def wait_recv_x(slot, j):
        for side in (0, 1):
            @pl.when(has_source(side))
            def _(side=side):
                x_copy(slot, side, j, T.at[slot, 1 + j, X if side == 0 else 1]).wait_recv()

    def relay_copy(step, p, target, side):
        slot = lax.rem(step, 2)
        j = Y - 1 - p
        land = 0 if side == 0 else X + 1
        return remote(rbuf.at[step, p], T.at[slot, 1 + j, land], rs_sem.at[step, p],
                      xr_sem.at[slot, side, j], {"lon": jnp.int32(target)})

    def do_relay(step, p):
        for source, relay, target, side in routes:
            @pl.when(lon == relay)
            def _(target=target, side=side):
                remote(rbuf.at[step, p], rbuf.at[step, p], rs_in_sem.at[0],
                       rr_sem.at[step, p], {"lon": jnp.int32(target)}).wait_recv()
                relay_copy(step, p, target, side).start()

    def y_copy(slot, side):
        if side == 0:
            return remote(T.at[slot, Y, pl.ds(1, X)], T.at[slot, 0, pl.ds(1, X)],
                          ys_sem.at[slot, 0], yr_sem.at[slot, 0], {"lat": lat + 1})
        return remote(T.at[slot, 1, pl.ds(1, X)], T.at[slot, Y + 1, pl.ds(1, X)],
                      ys_sem.at[slot, 1], yr_sem.at[slot, 1], {"lat": lat - 1})

    def y_target(side):
        return lat < lats - 1 if side == 0 else lat > 0

    def y_source(side):
        return lat > 0 if side == 0 else lat < lats - 1

    def z_copy(slot, side, j):
        other = lev + 1 if side == 0 else lev - 1
        return remote(zs.at[slot, side, j], zh.at[slot, side, j], zs_sem.at[slot, side, j],
                      zr_sem.at[slot, side, j], {"lev": other})

    def z_target(side):
        return lev < levs - 1 if side == 0 else lev > 0

    def z_source(side):
        return lev > 0 if side == 0 else lev < levs - 1

    def send_z(slot, j):
        for side in (0, 1):
            @pl.when(z_target(side))
            def _(side=side):
                z_copy(slot, side, j).start()

    def wait_send_z(slot, j):
        for side in (0, 1):
            @pl.when(z_target(side))
            def _(side=side):
                z_copy(slot, side, j).wait_send()

    def wait_recv_z(slot, j):
        for side in (0, 1):
            @pl.when(z_source(side))
            def _(side=side):
                z_copy(slot, side, j).wait_recv()

    def first_x(p, _):
        for j, relayed in ((p, False), (Y - 1 - p, True)):
            send_x(0, 0, j, p, relayed, (heat.at[j, X - 1], heat.at[j, 0]))
        return 0

    lax.fori_loop(0, pairs, first_x, 0)

    def wait_heat(j, _):
        load(j, 3).wait()
        return 0

    lax.fori_loop(0, Y, wait_heat, 0)
    for side in (0, 1):
        @pl.when(y_target(side))
        def _(side=side):
            y_copy(0, side).start()

    def first_z(j, _):
        for x in range(X):
            zs[0, 0, j, pl.ds(x, 1)] = T[0, 1 + j, 1 + x, pl.ds(Z - 1, 1)]
            zs[0, 1, j, pl.ds(x, 1)] = T[0, 1 + j, 1 + x, pl.ds(0, 1)]
        return 0

    lax.fori_loop(0, Y, first_z, 0)

    def first_z_send(j, _):
        send_z(0, j)
        return 0

    lax.fori_loop(0, Y, first_z_send, 0)

    level = lax.broadcasted_iota(jnp.int32, (Z, L), 0)

    def update(old, j, with_total):
        new = 1 - old
        total = None
        for x in range(X):
            c = T[old, 1 + j, 1 + x]
            ym, yp = T[old, j, 1 + x], T[old, j + 2, 1 + x]
            xm, xp = T[old, 1 + j, x], T[old, 1 + j, x + 2]
            zm = jnp.where(level == 0, zh[old, 0, j, pl.ds(x, 1)], pltpu.roll(c, 1, 0))
            zp = jnp.where(level == Z - 1, zh[old, 1, j, pl.ds(x, 1)], pltpu.roll(c, Z - 1, 0))
            spread = ym + yp + xm + xp + zm + zp - 6.0 * c
            value = (c - W[0, j, x] * (yp - ym) - W[1, j, x] * (xp - xm)
                     - W[2, j, x] * (zp - zm) + RATE * spread)
            T[new, 1 + j, 1 + x] = value
            if not with_total:
                zs[new, 0, j, pl.ds(x, 1)] = value[Z - 1:Z]
                zs[new, 1, j, pl.ds(x, 1)] = value[0:1]
            elif total is None:
                total = value
            else:
                total = total + value
        if with_total:
            tot[j] = total

    def arrivals(old, j, p, edge_side):
        wait_recv_x(old, j)
        wait_recv_z(old, j)

        @pl.when(jnp.logical_and(p == 0, y_source(edge_side)))
        def _():
            y_copy(old, edge_side).wait_recv()

    def departures(slot, j, p, edge_side):
        wait_send_x(slot, j)
        wait_send_z(slot, j)

        @pl.when(jnp.logical_and(p == 0, y_target(edge_side)))
        def _():
            y_copy(slot, edge_side).wait_send()

    def one_pair(q, _):
        step = q // pairs
        p = lax.rem(q, pairs)
        old = lax.rem(step, 2)
        new = 1 - old

        @pl.when(step == 0)
        def _():
            do_relay(0, p)
            for k in range(3):
                load(p, k).wait()
                load(Y - 1 - p, k).wait()

        for j, edge_side, relayed in ((p, 0, False), (Y - 1 - p, 1, True)):
            arrivals(old, j, p, edge_side)

            @pl.when(step > 0)
            def _(j=j, edge_side=edge_side):
                departures(new, j, p, 1 - edge_side)

            update(old, j, False)
            send_x(step + 1, new, j, p, relayed, (T.at[new, 1 + j, X], T.at[new, 1 + j, 1]))
            send_z(new, j)

            @pl.when(jnp.logical_and(p == 0, y_target(1 - edge_side)))
            def _(edge_side=edge_side):
                y_copy(new, 1 - edge_side).start()

        late = q - LAG

        @pl.when(late >= 0)
        def _():
            do_relay(late // pairs + 1, lax.rem(late, pairs))

        return 0

    lax.fori_loop(0, (STEPS - 1) * pairs, one_pair, 0)

    old = (STEPS - 1) % 2
    new = 1 - old

    def out_copy(j):
        return pltpu.make_async_copy(T.at[new, 1 + j, pl.ds(1, X)], end_out.at[j], out_sem.at[j])

    def t_copy(j):
        return remote(tot.at[j], ent.at[j], ts_sem.at[j], tr_sem.at[j], {"lon": lon + 1})

    def enter_copy(j):
        return pltpu.make_async_copy(ent.at[j], enter_out.at[j], enter_sem.at[j])

    def pass_total(p):
        for j in (p, Y - 1 - p):
            @pl.when(lon > 0)
            def _(j=j):
                t_copy(j).wait_recv()

                @pl.when(lon < lons - 1)
                def _():
                    tot[j] = tot[j] + ent[j]
                    t_copy(j).start()

            enter_copy(j).start()

    def clear_enter(j, _):
        ent[j] = jnp.zeros((Z, L), jnp.float32)
        return 0

    @pl.when(lon == 0)
    def _():
        lax.fori_loop(0, Y, clear_enter, 0)

    def leftover(p, _):
        do_relay(STEPS - 1, p)
        return 0

    lax.fori_loop(pairs - LAG, pairs, leftover, 0)

    def last_pair(p, _):
        for j, edge_side in ((p, 0), (Y - 1 - p, 1)):
            arrivals(old, j, p, edge_side)
            departures(new, j, p, 1 - edge_side)
            update(old, j, True)
        for j in (p, Y - 1 - p):
            @pl.when(jnp.logical_and(lon == 0, lons > 1))
            def _(j=j):
                t_copy(j).start()

            out_copy(j).start()

        @pl.when(p >= TOTAL_LAG)
        def _():
            pass_total(p - TOTAL_LAG)

        return 0

    lax.fori_loop(0, pairs, last_pair, 0)

    def last_totals(p, _):
        pass_total(p)
        return 0

    lax.fori_loop(max(pairs - TOTAL_LAG, 0), pairs, last_totals, 0)

    def drain(j, _):
        wait_send_x(old, j)
        wait_send_z(old, j)

        @pl.when(lon < lons - 1)
        def _():
            t_copy(j).wait_send()

        out_copy(j).wait()
        enter_copy(j).wait()
        return 0

    lax.fori_loop(0, Y, drain, 0)
    for side in (0, 1):
        @pl.when(y_target(side))
        def _(side=side):
            y_copy(old, side).wait_send()

    for source, relay, target, side in routes:
        def close(p, _, target=target, side=side):
            for step in range(STEPS):
                relay_copy(step, p, target, side).wait_send()
            return 0

        @pl.when(lon == relay)
        def _(close=close):
            lax.fori_loop(0, pairs, close, 0)


def integrate(scale, end_ref, enter_ref, acc_ref, copy_ref):
    X = end_ref.shape[1]
    running = enter_ref[0]
    for x in range(X):
        value = end_ref[0, x]
        copy_ref[0, x] = value
        running = running + value
        acc_ref[0, x] = running * scale


def per_device(routes, sizes, heat, north, east, vert):
    Y, X, Z, L = heat.shape
    pairs = Y // 2
    f32 = jnp.float32
    any_spec = pl.BlockSpec(memory_space=pl.ANY)
    dma = pltpu.SemaphoreType.DMA
    relay_rows = (STEPS, pairs) if routes else (1, 1)
    end, enter = pl.pallas_call(
        functools.partial(march, routes, sizes),
        out_shape=(jax.ShapeDtypeStruct((Y, X, Z, L), f32), jax.ShapeDtypeStruct((Y, Z, L), f32)),
        in_specs=[any_spec] * 4,
        out_specs=(any_spec, any_spec),
        scratch_shapes=[
            pltpu.VMEM((2, Y + 2, X + 2, Z, L), f32),
            pltpu.VMEM((3, Y, X, Z, L), f32),
            pltpu.VMEM((2, 2, Y, X, L), f32),
            pltpu.VMEM((2, 2, Y, X, L), f32),
            pltpu.VMEM((Y, Z, L), f32),
            pltpu.VMEM((Y, Z, L), f32),
            pltpu.VMEM(relay_rows + (Z, L), f32),
            dma((4, Y)),
            dma((2, 2, Y)), dma((2, 2, Y)),
            dma((2, 2)), dma((2, 2)),
            dma((2, 2, Y)), dma((2, 2, Y)),
            dma((1,)), dma(relay_rows), dma(relay_rows),
            dma((Y,)), dma((Y,)), dma((Y,)), dma((Y,)),
        ],
        compiler_params=pltpu.CompilerParams(
            collective_id=0, has_side_effects=True, vmem_limit_bytes=62 * 1024 * 1024),
        name="march",
    )(heat, north, east, vert)
    row = pl.BlockSpec((1, X, Z, L), lambda j: (j, 0, 0, 0))
    return pl.pallas_call(
        functools.partial(integrate, 1.0 / (X * sizes[1])),
        grid=(Y,),
        in_specs=[row, pl.BlockSpec((1, Z, L), lambda j: (j, 0, 0))],
        out_specs=(row, row),
        out_shape=(jax.ShapeDtypeStruct((Y, X, Z, L), f32),) * 2,
        name="integrate",
    )(end, enter)


def solution(mesh):
    spec = P("lat", "lon", "lev", None)
    sizes = tuple(mesh.shape[a] for a in ("lat", "lon", "lev"))
    return jax.shard_map(
        functools.partial(per_device, relay_routes(mesh), sizes),
        mesh=mesh, in_specs=(spec,) * 4, out_specs=(spec, spec), check_vma=False)
```

```python
import functools

import jax
import jax.numpy as jnp
from jax import lax
from jax.experimental import pallas as pl
from jax.experimental.pallas import tpu as pltpu
from jax.sharding import PartitionSpec as P

STEPS = 6
RATE = 0.05
LAG = 1
TOTAL_LAG = 4
RELAY = True
RELAY_FIRST_DIM = True
MESH = pl.DeviceIdType.MESH


def relay_routes(mesh):
    if not RELAY:
        return ()
    row = mesh.devices[0, :, 0]
    spots = [getattr(device, "coords", None) for device in row]
    if any(spot is None for spot in spots):
        return ()
    spots = [tuple(spot) for spot in spots]
    routes = []
    for low in range(len(spots) - 1):
        for source, target, side in ((low, low + 1, 0), (low + 1, low, 1)):
            a, b = spots[source], spots[target]
            differ = [d for d in range(3) if a[d] != b[d]]
            if len(differ) != 2:
                continue
            keep, change = differ if RELAY_FIRST_DIM else differ[::-1]
            corner = list(a)
            corner[change] = b[change]
            if tuple(corner) in spots:
                routes.append((source, spots.index(tuple(corner)), target, side))
    return tuple(routes)


def march(routes, sizes, heat, north, east, vert, end_out, enter_out,
          T, W, zh, zs, tot, ent, rbuf,
          load_sem, xs_sem, xr_sem, ys_sem, yr_sem, zs_sem, zr_sem,
          rs_in_sem, rr_sem, rs_sem, ts_sem, tr_sem, out_sem, enter_sem):
    lats, lons, levs = sizes
    Y, X, Z, L = heat.shape
    pairs = Y // 2
    lat, lon, lev = (lax.axis_index(a) for a in ("lat", "lon", "lev"))
    winds = (north, east, vert)

    def remote(src, dst, send, recv, where):
        return pltpu.make_async_remote_copy(
            src_ref=src, dst_ref=dst, send_sem=send, recv_sem=recv,
            device_id=where, device_id_type=MESH)

    def load(j, k):
        if k == 3:
            return pltpu.make_async_copy(heat.at[j], T.at[0, 1 + j, pl.ds(1, X)], load_sem.at[3, j])
        return pltpu.make_async_copy(winds[k].at[j], W.at[k, j], load_sem.at[k, j])

    def start_loads(p, _):
        for k in range(3):
            load(p, k).start()
            load(Y - 1 - p, k).start()
        return 0

    def start_heat(j, _):
        load(j, 3).start()
        return 0

    lax.fori_loop(0, Y, start_heat, 0)
    lax.fori_loop(0, pairs, start_loads, 0)

    @pl.when(lon == 0)
    def _():
        T[:, pl.ds(1, Y), 0] = jnp.zeros((2, Y, Z, L), jnp.float32)

    @pl.when(lon == lons - 1)
    def _():
        T[:, pl.ds(1, Y), X + 1] = jnp.zeros((2, Y, Z, L), jnp.float32)

    @pl.when(lat == 0)
    def _():
        T[:, 0, pl.ds(1, X)] = jnp.zeros((2, X, Z, L), jnp.float32)

    @pl.when(lat == lats - 1)
    def _():
        T[:, Y + 1, pl.ds(1, X)] = jnp.zeros((2, X, Z, L), jnp.float32)

    @pl.when(lev == 0)
    def _():
        zh[:, 0] = jnp.zeros((2, Y, X, L), jnp.float32)

    @pl.when(lev == levs - 1)
    def _():
        zh[:, 1] = jnp.zeros((2, Y, X, L), jnp.float32)

    barrier = pltpu.get_barrier_semaphore()
    expected = jnp.int32(0)
    for axis, place, count in (("lat", lat, lats), ("lon", lon, lons), ("lev", lev, levs)):
        for cond, other in ((place > 0, place - 1), (place < count - 1, place + 1)):
            @pl.when(cond)
            def _(axis=axis, other=other):
                pl.semaphore_signal(barrier, inc=1, device_id={axis: other}, device_id_type=MESH)
            expected = expected + jnp.where(cond, 1, 0)
    met = set()
    links = [(low, low + 2) for low in range(lons - 2)]
    for source, relay, target, _ in routes:
        links += [(source, relay), (relay, target)]
    for a, b in links:
        link = (min(a, b), max(a, b))
        if link[1] - link[0] == 1 or link in met:
            continue
        met.add(link)
        for me, other in (link, link[::-1]):
            @pl.when(lon == me)
            def _(other=other):
                pl.semaphore_signal(barrier, inc=1, device_id={"lon": jnp.int32(other)}, device_id_type=MESH)
            expected = expected + jnp.where(lon == me, 1, 0)
    pl.semaphore_wait(barrier, expected)

    def x_copy(slot, side, j, src):
        land = 0 if side == 0 else X + 1
        other = lon + 1 if side == 0 else lon - 1
        return remote(src, T.at[slot, 1 + j, land], xs_sem.at[slot, side, j],
                      xr_sem.at[slot, side, j], {"lon": other})

    def has_target(side):
        return lon < lons - 1 if side == 0 else lon > 0

    def has_source(side):
        return lon > 0 if side == 0 else lon < lons - 1

    def on_route(side, relayed):
        hit = False
        if relayed:
            for source, _, _, s in routes:
                if s == side:
                    hit = jnp.logical_or(hit, lon == source)
        return hit

    def send_x(step, slot, j, p, relayed, srcs):
        for side in (0, 1):
            routed = on_route(side, relayed)

            @pl.when(jnp.logical_and(has_target(side), jnp.logical_not(routed)))
            def _(side=side):
                x_copy(slot, side, j, srcs[side]).start()

        if relayed:
            for number, (source, relay, target, side) in enumerate(routes):
                @pl.when(lon == source)
                def _(relay=relay, side=side):
                    remote(srcs[side], rbuf.at[step, p], xs_sem.at[slot, side, j],
                           rr_sem.at[step, p], {"lon": jnp.int32(relay)}).start()

    def wait_send_x(slot, j):
        for side in (0, 1):
            @pl.when(has_target(side))
            def _(side=side):
                x_copy(slot, side, j, T.at[slot, 1 + j, X if side == 0 else 1]).wait_send()

    def wait_recv_x(slot, j):
        for side in (0, 1):
            @pl.when(has_source(side))
            def _(side=side):
                x_copy(slot, side, j, T.at[slot, 1 + j, X if side == 0 else 1]).wait_recv()

    def relay_copy(step, p, target, side):
        slot = lax.rem(step, 2)
        j = Y - 1 - p
        land = 0 if side == 0 else X + 1
        return remote(rbuf.at[step, p], T.at[slot, 1 + j, land], rs_sem.at[step, p],
                      xr_sem.at[slot, side, j], {"lon": jnp.int32(target)})

    def do_relay(step, p):
        for source, relay, target, side in routes:
            @pl.when(lon == relay)
            def _(target=target, side=side):
                remote(rbuf.at[step, p], rbuf.at[step, p], rs_in_sem.at[0],
                       rr_sem.at[step, p], {"lon": jnp.int32(target)}).wait_recv()
                relay_copy(step, p, target, side).start()

    def y_copy(slot, side):
        if side == 0:
            return remote(T.at[slot, Y, pl.ds(1, X)], T.at[slot, 0, pl.ds(1, X)],
                          ys_sem.at[slot, 0], yr_sem.at[slot, 0], {"lat": lat + 1})
        return remote(T.at[slot, 1, pl.ds(1, X)], T.at[slot, Y + 1, pl.ds(1, X)],
                      ys_sem.at[slot, 1], yr_sem.at[slot, 1], {"lat": lat - 1})

    def y_target(side):
        return lat < lats - 1 if side == 0 else lat > 0

    def y_source(side):
        return lat > 0 if side == 0 else lat < lats - 1

    def z_copy(slot, side, j):
        other = lev + 1 if side == 0 else lev - 1
        return remote(zs.at[slot, side, j], zh.at[slot, side, j], zs_sem.at[slot, side, j],
                      zr_sem.at[slot, side, j], {"lev": other})

    def z_target(side):
        return lev < levs - 1 if side == 0 else lev > 0

    def z_source(side):
        return lev > 0 if side == 0 else lev < levs - 1

    def send_z(slot, j):
        for side in (0, 1):
            @pl.when(z_target(side))
            def _(side=side):
                z_copy(slot, side, j).start()

    def wait_send_z(slot, j):
        for side in (0, 1):
            @pl.when(z_target(side))
            def _(side=side):
                z_copy(slot, side, j).wait_send()

    def wait_recv_z(slot, j):
        for side in (0, 1):
            @pl.when(z_source(side))
            def _(side=side):
                z_copy(slot, side, j).wait_recv()

    def first_x(p, _):
        for j, relayed in ((p, False), (Y - 1 - p, True)):
            send_x(0, 0, j, p, relayed, (heat.at[j, X - 1], heat.at[j, 0]))
        return 0

    lax.fori_loop(0, pairs, first_x, 0)

    def wait_heat(j, _):
        load(j, 3).wait()
        return 0

    lax.fori_loop(0, Y, wait_heat, 0)
    for side in (0, 1):
        @pl.when(y_target(side))
        def _(side=side):
            y_copy(0, side).start()

    def first_z(j, _):
        for x in range(X):
            zs[0, 0, j, pl.ds(x, 1)] = T[0, 1 + j, 1 + x, pl.ds(Z - 1, 1)]
            zs[0, 1, j, pl.ds(x, 1)] = T[0, 1 + j, 1 + x, pl.ds(0, 1)]
        return 0

    lax.fori_loop(0, Y, first_z, 0)

    def first_z_send(j, _):
        send_z(0, j)
        return 0

    lax.fori_loop(0, Y, first_z_send, 0)

    level = lax.broadcasted_iota(jnp.int32, (Z, L), 0)

    def update(old, j, with_total):
        new = 1 - old
        total = None
        for x in range(X):
            c = T[old, 1 + j, 1 + x]
            ym, yp = T[old, j, 1 + x], T[old, j + 2, 1 + x]
            xm, xp = T[old, 1 + j, x], T[old, 1 + j, x + 2]
            zm = jnp.where(level == 0, zh[old, 0, j, pl.ds(x, 1)], pltpu.roll(c, 1, 0))
            zp = jnp.where(level == Z - 1, zh[old, 1, j, pl.ds(x, 1)], pltpu.roll(c, Z - 1, 0))
            spread = ym + yp + xm + xp + zm + zp - 6.0 * c
            value = (c - W[0, j, x] * (yp - ym) - W[1, j, x] * (xp - xm)
                     - W[2, j, x] * (zp - zm) + RATE * spread)
            T[new, 1 + j, 1 + x] = value
            if not with_total:
                zs[new, 0, j, pl.ds(x, 1)] = value[Z - 1:Z]
                zs[new, 1, j, pl.ds(x, 1)] = value[0:1]
            elif total is None:
                total = value
            else:
                total = total + value
        if with_total:
            tot[0, j] = total

    def arrivals(old, j, p, edge_side):
        wait_recv_x(old, j)
        wait_recv_z(old, j)

        @pl.when(jnp.logical_and(p == 0, y_source(edge_side)))
        def _():
            y_copy(old, edge_side).wait_recv()

    def departures(slot, j, p, edge_side):
        wait_send_x(slot, j)
        wait_send_z(slot, j)

        @pl.when(jnp.logical_and(p == 0, y_target(edge_side)))
        def _():
            y_copy(slot, edge_side).wait_send()

    def one_pair(q, _):
        step = q // pairs
        p = lax.rem(q, pairs)
        old = lax.rem(step, 2)
        new = 1 - old

        @pl.when(step == 0)
        def _():
            do_relay(0, p)
            for k in range(3):
                load(p, k).wait()
                load(Y - 1 - p, k).wait()

        for j, edge_side, relayed in ((p, 0, False), (Y - 1 - p, 1, True)):
            arrivals(old, j, p, edge_side)

            @pl.when(step > 0)
            def _(j=j, edge_side=edge_side):
                departures(new, j, p, 1 - edge_side)

            update(old, j, False)
            send_x(step + 1, new, j, p, relayed, (T.at[new, 1 + j, X], T.at[new, 1 + j, 1]))
            send_z(new, j)

            @pl.when(jnp.logical_and(p == 0, y_target(1 - edge_side)))
            def _(edge_side=edge_side):
                y_copy(new, 1 - edge_side).start()

        late = q - LAG

        @pl.when(late >= 0)
        def _():
            do_relay(late // pairs + 1, lax.rem(late, pairs))

        return 0

    lax.fori_loop(0, (STEPS - 1) * pairs, one_pair, 0)

    old = (STEPS - 1) % 2
    new = 1 - old

    def out_copy(j):
        return pltpu.make_async_copy(T.at[new, 1 + j, pl.ds(1, X)], end_out.at[j], out_sem.at[j])

    def near_copy(j):
        return remote(tot.at[0, j], ent.at[0, j], ts_sem.at[0, j], tr_sem.at[0, j], {"lon": lon + 1})

    def far_copy(j, which):
        return remote(tot.at[which, j], ent.at[1, j], ts_sem.at[1, j], tr_sem.at[1, j], {"lon": lon + 2})

    def enter_copy(j):
        return pltpu.make_async_copy(ent.at[0, j], enter_out.at[j], enter_sem.at[j])

    def pass_total(p):
        for j in (p, Y - 1 - p):
            @pl.when(lon > 0)
            def _(j=j):
                near_copy(j).wait_recv()

            @pl.when(lon > 1)
            def _(j=j):
                far_copy(j, 1).wait_recv()
                ent[0, j] = ent[0, j] + ent[1, j]

            @pl.when(jnp.logical_and(lon > 0, lon < lons - 2))
            def _(j=j):
                tot[1, j] = tot[0, j] + ent[0, j]
                far_copy(j, 1).start()

            enter_copy(j).start()

    def clear_enter(j, _):
        ent[0, j] = jnp.zeros((Z, L), jnp.float32)
        return 0

    @pl.when(lon == 0)
    def _():
        lax.fori_loop(0, Y, clear_enter, 0)

    def leftover(p, _):
        do_relay(STEPS - 1, p)
        return 0

    lax.fori_loop(pairs - LAG, pairs, leftover, 0)

    def last_pair(p, _):
        for j, edge_side in ((p, 0), (Y - 1 - p, 1)):
            arrivals(old, j, p, edge_side)
            departures(new, j, p, 1 - edge_side)
            update(old, j, True)
        for j in (p, Y - 1 - p):
            @pl.when(jnp.logical_and(lon == 0, lons > 2))
            def _(j=j):
                far_copy(j, 0).start()

            @pl.when(lon < lons - 1)
            def _(j=j):
                near_copy(j).start()

            out_copy(j).start()

        @pl.when(p >= TOTAL_LAG)
        def _():
            pass_total(p - TOTAL_LAG)

        return 0

    lax.fori_loop(0, pairs, last_pair, 0)

    def last_totals(p, _):
        pass_total(p)
        return 0

    lax.fori_loop(max(pairs - TOTAL_LAG, 0), pairs, last_totals, 0)

    def drain(j, _):
        wait_send_x(old, j)
        wait_send_z(old, j)

        @pl.when(lon < lons - 1)
        def _():
            near_copy(j).wait_send()

        @pl.when(lon < lons - 2)
        def _():
            far_copy(j, 1).wait_send()

        out_copy(j).wait()
        enter_copy(j).wait()
        return 0

    lax.fori_loop(0, Y, drain, 0)
    for side in (0, 1):
        @pl.when(y_target(side))
        def _(side=side):
            y_copy(old, side).wait_send()

    for source, relay, target, side in routes:
        def close(p, _, target=target, side=side):
            for step in range(STEPS):
                relay_copy(step, p, target, side).wait_send()
            return 0

        @pl.when(lon == relay)
        def _(close=close):
            lax.fori_loop(0, pairs, close, 0)


def integrate(scale, end_ref, enter_ref, acc_ref, copy_ref):
    X = end_ref.shape[1]
    running = enter_ref[0]
    for x in range(X):
        value = end_ref[0, x]
        copy_ref[0, x] = value
        running = running + value
        acc_ref[0, x] = running * scale


def per_device(routes, sizes, heat, north, east, vert):
    Y, X, Z, L = heat.shape
    pairs = Y // 2
    f32 = jnp.float32
    any_spec = pl.BlockSpec(memory_space=pl.ANY)
    dma = pltpu.SemaphoreType.DMA
    relay_rows = (STEPS, pairs) if routes else (1, 1)
    block = 4 * (Y + 2) * (X + 2) * Z * L
    grant = 5 * block + block // 8
    end, enter = pl.pallas_call(
        functools.partial(march, routes, sizes),
        out_shape=(jax.ShapeDtypeStruct((Y, X, Z, L), f32), jax.ShapeDtypeStruct((Y, Z, L), f32)),
        in_specs=[any_spec] * 4,
        out_specs=(any_spec, any_spec),
        scratch_shapes=[
            pltpu.VMEM((2, Y + 2, X + 2, Z, L), f32),
            pltpu.VMEM((3, Y, X, Z, L), f32),
            pltpu.VMEM((2, 2, Y, X, L), f32),
            pltpu.VMEM((2, 2, Y, X, L), f32),
            pltpu.VMEM((2, Y, Z, L), f32),
            pltpu.VMEM((2, Y, Z, L), f32),
            pltpu.VMEM(relay_rows + (Z, L), f32),
            dma((4, Y)),
            dma((2, 2, Y)), dma((2, 2, Y)),
            dma((2, 2)), dma((2, 2)),
            dma((2, 2, Y)), dma((2, 2, Y)),
            dma((1,)), dma(relay_rows), dma(relay_rows),
            dma((2, Y)), dma((2, Y)), dma((Y,)), dma((Y,)),
        ],
        compiler_params=pltpu.CompilerParams(
            collective_id=0, has_side_effects=True, vmem_limit_bytes=grant),
        name="march",
    )(heat, north, east, vert)
    row = pl.BlockSpec((1, X, Z, L), lambda j: (j, 0, 0, 0))
    return pl.pallas_call(
        functools.partial(integrate, 1.0 / (X * sizes[1])),
        grid=(Y,),
        in_specs=[row, pl.BlockSpec((1, Z, L), lambda j: (j, 0, 0))],
        out_specs=(row, row),
        out_shape=(jax.ShapeDtypeStruct((Y, X, Z, L), f32),) * 2,
        compiler_params=pltpu.CompilerParams(vmem_limit_bytes=8 * 1024 * 1024),
        name="integrate",
    )(end, enter)


def solution(mesh):
    spec = P("lat", "lon", "lev", None)
    sizes = tuple(mesh.shape[a] for a in ("lat", "lon", "lev"))
    return jax.shard_map(
        functools.partial(per_device, relay_routes(mesh), sizes),
        mesh=mesh, in_specs=(spec,) * 4, out_specs=(spec, spec), check_vma=False)
```
